8 devices in a mesh: dp: 1 (over z), ep2: 2 (over y), ep: 4 (over x, core).
Axes of the slice: x: 2, y: 2, z: 1, core: 2. Of those that a mesh axis runs over, the one named last changes fastest.
Arguments:
- tokens: bfloat16 [1024, 2048], P(('dp', 'ep2', 'ep'))
- expert_ids: int32 [1024, 8], P(('dp', 'ep2', 'ep'))
- gates: float32 [1024, 8], P(('dp', 'ep2', 'ep'))
- w_gate: bfloat16 [128, 2048, 768], P(('ep2', 'ep'))
- w_up: bfloat16 [128, 2048, 768], P(('ep2', 'ep'))
- w_down: bfloat16 [128, 768, 2048], P(('ep2', 'ep'))
Outputs:
- output: bfloat16 [1024, 2048], P(('dp', 'ep2', 'ep'))
All inputs are finite; a program needn't handle non-finite values.
Results may differ from the reference program's by a relative error of at most 0.0011.
Values are sent between devices in bfloat16 or wider.
A program may use at most 1 GiB of HBM per device.

```python
import jax
import jax.numpy as jnp
from jax import lax

MODEL_DIM = 2048
FFN_DIM = 768
NUM_EXPERTS = 128
TOP_K = 8
TOK_DEV = 128
GROUP_DEVS = 8


def random_perms(perm_key, n_rows, length):
    scores = jax.random.randint(perm_key, (n_rows, length), 0, 1048576) * length + jnp.arange(length)[None, :]
    return jnp.argsort(scores, axis=1, stable=True)


def draw_routing(route_key):
    local_count = NUM_EXPERTS // GROUP_DEVS
    key_dev, key_loc, key_tok, key_off = jax.random.split(route_key, 4)
    dev_perm = random_perms(key_dev, GROUP_DEVS, GROUP_DEVS)
    loc_perm = random_perms(key_loc, GROUP_DEVS, local_count)
    tok_perm = random_perms(key_tok, GROUP_DEVS, TOK_DEV)
    offset = jax.random.randint(key_off, (GROUP_DEVS, 1, 1), 0, NUM_EXPERTS)
    row_pos = offset + tok_perm[:, :, None] * TOP_K + jnp.arange(TOP_K)[None, None, :]
    row_mod = (row_pos % NUM_EXPERTS).reshape(GROUP_DEVS, TOK_DEV * TOP_K)
    dev_col = row_mod % GROUP_DEVS
    loc_col = row_mod // GROUP_DEVS
    dest_dev = jnp.take_along_axis(dev_perm, dev_col, axis=1)
    dest_loc = (jnp.take_along_axis(loc_perm, loc_col, axis=1) + dev_col) % local_count
    expert_ids = dest_dev * local_count + dest_loc
    return expert_ids.reshape(GROUP_DEVS * TOK_DEV, TOP_K).astype(jnp.int32)


def setup_inputs(seed: int = 0, part: int = 0) -> dict:
    base_key = jax.random.key(seed)
    part_key = jax.random.fold_in(base_key, part)
    key_x, key_route, key_gate = jax.random.split(part_key, 3)
    key_w1, key_w3, key_w2 = jax.random.split(base_key, 3)
    n_tok = GROUP_DEVS * TOK_DEV
    tokens = jax.random.normal(key_x, (n_tok, MODEL_DIM), jnp.float32).astype(jnp.bfloat16)
    expert_ids = draw_routing(key_route)
    gates = jax.nn.softmax(1.5 * jax.random.normal(key_gate, (n_tok, TOP_K), jnp.float32), axis=-1)
    w_gate = (jax.random.normal(key_w1, (NUM_EXPERTS, MODEL_DIM, FFN_DIM), jnp.float32) * MODEL_DIM ** -0.5).astype(jnp.bfloat16)
    w_up = (jax.random.normal(key_w3, (NUM_EXPERTS, MODEL_DIM, FFN_DIM), jnp.float32) * MODEL_DIM ** -0.5).astype(jnp.bfloat16)
    w_down = (jax.random.normal(key_w2, (NUM_EXPERTS, FFN_DIM, MODEL_DIM), jnp.float32) * (3.0 * FFN_DIM ** -0.5)).astype(jnp.bfloat16)
    return {'tokens': tokens, 'expert_ids': expert_ids, 'gates': gates, 'w_gate': w_gate, 'w_up': w_up, 'w_down': w_down}


def expert_rows(operands):
    rows, w_one, w_three, w_two = operands
    act_gate = jnp.dot(rows, w_one, preferred_element_type=jnp.float32)
    act_up = jnp.dot(rows, w_three, preferred_element_type=jnp.float32)
    hidden = (jax.nn.silu(act_gate) * act_up).astype(jnp.bfloat16)
    return jnp.dot(hidden, w_two, preferred_element_type=jnp.float32).astype(jnp.bfloat16)


def reference(tokens, expert_ids, gates, w_gate, w_up, w_down):
    n_tok = tokens.shape[0]
    n_rows = n_tok * TOP_K
    per_expert = GROUP_DEVS * ((TOK_DEV * TOP_K + NUM_EXPERTS - 1) // NUM_EXPERTS)
    flat_ids = expert_ids.reshape(n_rows)
    sort_order = jnp.argsort(flat_ids, stable=True)
    counts = jnp.bincount(flat_ids, length=NUM_EXPERTS)
    starts = jnp.cumsum(counts) - counts
    rank_sorted = (jnp.arange(n_rows) - starts[flat_ids[sort_order]]).astype(jnp.int32)
    row_rank = jnp.zeros((n_rows,), jnp.int32).at[sort_order].set(rank_sorted)
    dest_pos = flat_ids * per_expert + row_rank
    buffer = jnp.zeros((NUM_EXPERTS * per_expert, MODEL_DIM), tokens.dtype).at[dest_pos].set(jnp.repeat(tokens, TOP_K, axis=0))
    expert_out = lax.map(expert_rows, (buffer.reshape(NUM_EXPERTS, per_expert, MODEL_DIM), w_gate, w_up, w_down))
    picked = expert_out.reshape(NUM_EXPERTS * per_expert, MODEL_DIM)[dest_pos].reshape(n_tok, TOP_K, MODEL_DIM)
    total = tokens.astype(jnp.float32)
    for slot_j in range(TOP_K):
        total = total + gates[:, slot_j:slot_j + 1] * picked[:, slot_j].astype(jnp.float32)
    return total.astype(jnp.bfloat16)
```

```python
import functools

import jax
import jax.numpy as jnp
from jax import lax
from jax.experimental import pallas as pl
from jax.experimental.pallas import tpu as pltpu
from jax.sharding import PartitionSpec as P

N_DEV = 8
N_TOK = 128
N_TOP = 8
DIM = 2048
FFN = 768
N_EXP = 128
N_LOC = 16
CAP = 8
RING = 5
CHUNKS = 4
CHUNK_ROWS = N_TOK // CHUNKS
N_PAIR = N_LOC // 2
BF16 = jnp.bfloat16
F32 = jnp.float32

OFFSETS = ((1, 1, 0), (1, 1, 1), (1, 0, 0), (0, 1, 0), (1, 0, 1), (0, 1, 1), (0, 0, 1))


def iota(shape, axis):
    return lax.broadcasted_iota(jnp.int32, shape, axis)


def dot(a, b):
    return jnp.dot(a, b, preferred_element_type=F32)


def moe_kernel(tok, ids_t, ids, gates, w1, w3, w2, out,
               xall, xg, yrecv, acc, pm, gm, w1b, w3b, w2b, idsall,
               sem_w, sem_tok, ids_send, ids_recv, ag_send, ag_recv, y_send, y_recv):
    dp = lax.axis_index('dp')
    gy = lax.axis_index('ep2')
    ep = lax.axis_index('ep')
    gx, gc = ep // 2, ep % 2
    me = gy * 4 + ep

    def flip(v, d):
        return v + d * (1 - 2 * v)

    def index_of(off):
        dx, dy, dc = off
        return flip(gy, dy) * 4 + flip(gx, dx) * 2 + flip(gc, dc)

    def mesh_id(idx):
        return (dp, idx // 4, idx % 4)

    def weight_copy(e, which):
        slot = e % RING
        source, ring = ((w1, w1b), (w3, w3b), (w2, w2b))[which]
        return pltpu.make_async_copy(source.at[e], ring.at[slot], sem_w.at[which, slot])

    tok_copy = pltpu.make_async_copy(tok, xall.at[me], sem_tok)
    tok_copy.start()
    for e in range(RING):
        for which in range(3):
            weight_copy(e, which).start()

    barrier = pltpu.get_barrier_semaphore()
    for off in OFFSETS:
        pl.semaphore_signal(barrier, inc=1, device_id=mesh_id(index_of(off)),
                            device_id_type=pl.DeviceIdType.MESH)
    pl.semaphore_wait(barrier, len(OFFSETS))

    def ids_copy(r, owner, dest):
        return pltpu.make_async_remote_copy(
            src_ref=ids_t, dst_ref=idsall.at[owner], send_sem=ids_send.at[r], recv_sem=ids_recv.at[r],
            device_id=mesh_id(dest), device_id_type=pl.DeviceIdType.MESH)

    for r, off in enumerate(OFFSETS):
        ids_copy(r, me, index_of(off)).start()

    partner = index_of((0, 0, 1))
    x_next = index_of((1, 0, 0))
    y_next = index_of((0, 1, 0))
    diag = index_of((1, 1, 0))
    relay_from = x_next + gc * (y_next - x_next)
    relay_to = y_next + gc * (x_next - y_next)

    def tok_send(shard, q, kind, dest):
        rows = pl.ds(q * CHUNK_ROWS, CHUNK_ROWS)
        return pltpu.make_async_remote_copy(
            src_ref=xall.at[shard, rows], dst_ref=xall.at[shard, rows],
            send_sem=ag_send.at[kind, q], recv_sem=ag_recv.at[shard, q],
            device_id=mesh_id(dest), device_id_type=pl.DeviceIdType.MESH)

    tok_copy.wait()
    for q in range(CHUNKS):
        tok_send(me, q, 1, x_next).start()
        tok_send(me, q, 2, y_next).start()
    for q in range(CHUNKS):
        tok_send(me, q, 0, partner).start()

    acc[...] = xall[me].astype(F32)
    idsall[me] = ids_t[...]

    gate_exp = jnp.zeros((N_TOK, N_EXP), F32)
    hot = jnp.zeros((N_TOK, N_EXP), F32)
    lane = iota((N_TOK, N_EXP), 1)
    for j in range(N_TOP):
        same = ids[:, j:j + 1] == lane
        gate_exp = gate_exp + jnp.where(same, gates[:, j:j + 1], 0.0)
        hot = hot + jnp.where(same, 1.0, 0.0)
    low = (iota((N_TOK, N_TOK), 1) < iota((N_TOK, N_TOK), 0)).astype(F32).astype(BF16)
    rank = dot(low, hot.astype(BF16))
    slot_of = jnp.where(hot > 0.5, rank, -1.0)
    g1 = gate_exp.astype(BF16)
    rest = gate_exp - g1.astype(F32)
    g2 = rest.astype(BF16)
    g3 = (rest - g2.astype(F32)).astype(BF16)
    stacked = jnp.concatenate([slot_of.astype(BF16), g1, g2, g3], axis=0)
    for p in range(N_PAIR):
        col = iota((N_EXP, N_TOK), 1)
        expert = (col // 16) * N_LOC + 2 * p + (col // 8) % 2
        spread = (iota((N_EXP, N_TOK), 0) == expert).astype(F32).astype(BF16)
        wide = dot(stacked, spread)
        keep = wide[:N_TOK] == (iota((N_TOK, N_TOK), 1) % CAP).astype(F32)
        for part in range(3):
            piece = wide[(part + 1) * N_TOK:(part + 2) * N_TOK]
            gm[part, :, p * N_TOK:(p + 1) * N_TOK] = jnp.where(keep, piece, 0.0).astype(BF16)

    for r, off in enumerate(OFFSETS):
        ids_copy(r, index_of(off), index_of(off)).wait_recv()
    expert_row = me * N_LOC + iota((N_LOC, N_TOK), 0)
    hots = []
    for s in range(N_DEV):
        any_hit = jnp.zeros((N_LOC, N_TOK), F32)
        for j in range(N_TOP):
            any_hit = any_hit + jnp.where(idsall[s, j:j + 1, :] == expert_row, 1.0, 0.0)
        hots.append(any_hit)
    hot_t = jnp.concatenate(hots, axis=0)
    up = (iota((N_TOK, N_TOK), 0) < iota((N_TOK, N_TOK), 1)).astype(F32).astype(BF16)
    slot_t = jnp.where(hot_t > 0.5, dot(hot_t.astype(BF16), up), -1.0).astype(BF16)
    for k in range(4):
        row = iota((256, N_TOK), 0)
        source = 2 * k + (row // 8) % 2
        spread = (iota((256, N_TOK), 1) == source * N_LOC + row // 16).astype(F32).astype(BF16)
        wide = dot(spread, slot_t)
        one = jnp.where(wide == (row % CAP).astype(F32), 1.0, 0.0)
        left = jnp.where((row // 8) % 2 == 0, one, 0.0)
        right = one - left
        pm[k, :, :N_TOK] = left.astype(BF16)
        pm[k, :, N_TOK:] = right.astype(BF16)

    def gather(chip):
        rows = xall[pl.ds(chip * 2, 2)].reshape(2 * N_TOK, DIM)
        for n in range(0, DIM, 512):
            xg[chip, :, n:n + 512] = dot(pm[chip], rows[:, n:n + 512]).astype(BF16)

    def wait_tok(shard, q):
        tok_send(shard, q, 0, partner).wait_recv()

    for q in range(CHUNKS):
        wait_tok(relay_from, q)
        tok_send(relay_from, q, 4, relay_to).start()
        tok_send(relay_from, q, 3, partner).start()
        wait_tok(relay_to, q)
        tok_send(relay_to, q, 5, partner).start()
        if q == 1:
            for qq in range(CHUNKS):
                wait_tok(partner, qq)
            gather(me // 2)
    for q in range(CHUNKS):
        wait_tok(diag, q)
        tok_send(diag, q, 6, partner).start()
        if q == 0:
            for qq in range(CHUNKS):
                wait_tok(index_of((1, 0, 1)), qq)
                wait_tok(index_of((0, 1, 1)), qq)
            gather(x_next // 2)
            gather(y_next // 2)
    for q in range(CHUNKS):
        wait_tok(index_of((1, 1, 1)), q)
    gather(diag // 2)

    for q in range(CHUNKS):
        tok_send(me, q, 0, partner).wait_send()
        tok_send(me, q, 1, x_next).wait_send()
        tok_send(me, q, 2, y_next).wait_send()
        tok_send(relay_from, q, 3, partner).wait_send()
        tok_send(relay_from, q, 4, relay_to).wait_send()
        tok_send(relay_to, q, 5, partner).wait_send()
        tok_send(diag, q, 6, partner).wait_send()
    for r, off in enumerate(OFFSETS):
        ids_copy(r, me, index_of(off)).wait_send()

    def y_copy(p, r, owner, dest):
        return pltpu.make_async_remote_copy(
            src_ref=xall.at[p, pl.ds(dest * 16, 16)], dst_ref=yrecv.at[p, pl.ds(owner * 16, 16)],
            send_sem=y_send.at[p, r], recv_sem=y_recv.at[p, r],
            device_id=mesh_id(dest), device_id_type=pl.DeviceIdType.MESH)

    def refill(e, which):
        @pl.when(e + RING < N_LOC)
        def _():
            weight_copy(e + RING, which).start()

    def pair_step(p, _):
        hidden = []
        for half in range(2):
            e = 2 * p + half
            slot = e % RING
            rows = jnp.concatenate(
                [xg[k, pl.ds(pl.multiple_of(e * 16, 16), 16), :] for k in range(4)], axis=0)
            weight_copy(e, 0).wait()
            act_gate = dot(rows, w1b[slot])
            refill(e, 0)
            weight_copy(e, 1).wait()
            act_up = dot(rows, w3b[slot])
            refill(e, 1)
            hidden.append((act_gate * jax.nn.sigmoid(act_gate) * act_up).astype(BF16))
        for half in range(2):
            weight_copy(2 * p + half, 2).wait()
        for n in range(0, DIM, 512):
            parts = []
            for half in range(2):
                slot = (2 * p + half) % RING
                parts.append(dot(hidden[half], w2b[slot, :, n:n + 512]).reshape(N_DEV, CAP, 512))
            both = jnp.concatenate(parts, axis=1).reshape(N_TOK, 512)
            xall[p, :, n:n + 512] = both.astype(BF16)
        for half in range(2):
            refill(2 * p + half, 2)
        mine = pl.ds(pl.multiple_of(me * 16, 16), 16)
        yrecv[p, mine, :] = xall[p, mine, :]
        for r, off in enumerate(OFFSETS):
            y_copy(p, r, me, index_of(off)).start()
        return 0

    lax.fori_loop(0, N_PAIR, pair_step, 0)

    def combine(h, _):
        for r, off in enumerate(OFFSETS):
            y_copy(2 * h, r, index_of(off), index_of(off)).wait_recv()
            y_copy(2 * h + 1, r, index_of(off), index_of(off)).wait_recv()
        cols = pl.ds(pl.multiple_of(h * 256, 256), 256)
        for n in range(0, DIM, 512):
            rows = yrecv[pl.ds(2 * h, 2), :, n:n + 512].reshape(256, 512)
            total = dot(gm[0, :, cols], rows) + dot(gm[1, :, cols], rows) + dot(gm[2, :, cols], rows)
            acc[:, n:n + 512] += total
        return 0

    lax.fori_loop(0, N_PAIR // 2, combine, 0)
    out[...] = acc[...].astype(BF16)

    def drain(p, _):
        for r, off in enumerate(OFFSETS):
            y_copy(p, r, me, index_of(off)).wait_send()
        return 0

    lax.fori_loop(0, N_PAIR, drain, 0)


def solution(mesh):
    group_axes = ('ep2', 'ep')
    row_spec = P(('dp', 'ep2', 'ep'), None)
    weight_spec = P(group_axes, None, None)

    def device_step(tokens, expert_ids, gates, w_gate, w_up, w_down):
        vmem = pl.BlockSpec(memory_space=pltpu.VMEM)
        hbm = pl.BlockSpec(memory_space=pl.ANY)
        dma = pltpu.SemaphoreType.DMA
        return pl.pallas_call(
            moe_kernel,
            out_shape=jax.ShapeDtypeStruct((N_TOK, DIM), BF16),
            in_specs=[hbm, vmem, vmem, vmem, hbm, hbm, hbm],
            out_specs=vmem,
            scratch_shapes=[
                pltpu.VMEM((N_DEV, N_TOK, DIM), BF16),
                pltpu.VMEM((4, 256, DIM), BF16),
                pltpu.VMEM((N_PAIR, N_TOK, DIM), BF16),
                pltpu.VMEM((N_TOK, DIM), F32),
                pltpu.VMEM((4, 256, 256), BF16),
                pltpu.VMEM((3, N_TOK, N_EXP * CAP), BF16),
                pltpu.VMEM((RING, DIM, FFN), BF16),
                pltpu.VMEM((RING, DIM, FFN), BF16),
                pltpu.VMEM((RING, FFN, DIM), BF16),
                pltpu.VMEM((N_DEV, N_TOP, N_TOK), jnp.int32),
                dma((3, RING)),
                dma,
                dma((7,)),
                dma((7,)),
                dma((7, CHUNKS)),
                dma((N_DEV, CHUNKS)),
                dma((N_PAIR, 7)),
                dma((N_PAIR, 7)),
            ],
            compiler_params=pltpu.CompilerParams(
                collective_id=0, has_side_effects=True, vmem_limit_bytes=67043328),
            name='moe_step',
        )(tokens, expert_ids.T, expert_ids, gates, w_gate, w_up, w_down)

    return jax.shard_map(device_step, mesh=mesh,
                         in_specs=(row_spec, row_spec, row_spec, weight_spec, weight_spec, weight_spec),
                         out_specs=row_spec, check_vma=False)
```
